32 devices in a mesh: tm: 8 (over z, x), lev: 4 (over y, core).
Axes of the slice: x: 2, y: 2, z: 4, core: 2. Of those that a mesh axis runs over, the one named last changes fastest.
Arguments:
- increment: float32 [8, 3, 8, 256, 512], P('tm', None, 'lev'), may hold values from -6 to 6
- multiplier: float32 [8, 3, 8, 256, 512], P('tm', None, 'lev'), may hold values from -6 to 6
- error_var: float32 [8, 3, 8, 256, 512], P('tm', None, 'lev'), may hold values from 0.1 to 1
- obs_cell: int32 [8, 8, 512], P('tm', 'lev'), may hold values from 0 to 131071
- obs_dual: float32 [8, 8, 512], P('tm', 'lev'), may hold values from -6 to 6
- obs_var: float32 [8, 8, 512], P('tm', 'lev'), may hold values from 0.5 to 2
- level_gain: float32 [8], P('lev'), may hold values from 0.5 to 1.5
- mean_depth: float32 [8], P('lev'), may hold values from 0.5 to 2
- chain_decay: float32 [8, 3, 8], P('tm', None, 'lev'), may hold values from 0 to 1
Outputs:
- dual_product: float32 [8, 3, 8, 256, 512], P('tm', None, 'lev')
- obs_product: float32 [8, 8, 512], P('tm', 'lev')
- state_block_product: float32 [8, 3, 8, 256, 512], P('tm', None, 'lev')
- chain_solution: float32 [8, 3, 8, 256, 512], P('tm', None, 'lev')
The draws below stay inside these ranges and needn't reach their ends.
All inputs are finite; a program needn't handle non-finite values.
Results may differ from the reference program's by a relative error of at most 0.0001.
Values sent between devices are 32-bit elements; how exact they have to be, the bound alone decides.
A program may use at most 320 MiB of HBM per device.

```python
import math
import jax
import jax.numpy as jnp
from jax import lax

GX = 256
GY = 512
STEPS = 2
NOBS = 512
WINDOW_PIECES = 8
LEVELS = 8


def draw_chain_decay(key, part):
    key_slow = jax.random.fold_in(key, 11)
    key_base = jax.random.fold_in(key, 12)
    key_jitter = jax.random.fold_in(key, 13)
    pulse_seed_handle = jax.random.fold_in(key, 14)
    key_depth = jax.random.fold_in(key, 15)
    slow_share = 0.5
    slow = jax.random.uniform(key_slow, (3, LEVELS), jnp.float32) < slow_share
    fast_rate = jnp.exp(jax.random.uniform(key_base, (3, LEVELS), jnp.float32, jnp.log(0.5), jnp.log(1.5)))
    slow_rate = jnp.full((3, LEVELS), -jnp.log(0.3) / WINDOW_PIECES, jnp.float32)
    base = jnp.where(slow, slow_rate, fast_rate)
    jitter = jax.random.uniform(key_jitter, (WINDOW_PIECES, 3, LEVELS), jnp.float32, 0.5, 1.5)
    scale_multiplier = jnp.exp(-base[None] * jitter)
    piece_pulses_sampled = jax.random.randint(pulse_seed_handle, (2,), 0, WINDOW_PIECES)
    measured_positions = jnp.arange(WINDOW_PIECES)
    measured_indicator = jnp.any(measured_positions[:, None] == piece_pulses_sampled[None, :], axis=1)
    depth_draw = jax.random.uniform(key_depth, (WINDOW_PIECES, 3, LEVELS), jnp.float32, 0.5, 0.8)
    return jnp.where(measured_indicator[:, None, None], scale_multiplier * depth_draw, scale_multiplier)


def set_ends(values, stream_key, least, top_value):
    longest = values.shape.index(max(values.shape))
    spots = []
    for shift in (0, 1):
        where = [jax.random.randint(jax.random.fold_in(stream_key, axis), (), 0, length) for axis, length in enumerate(values.shape)]
        where[longest] = (where[longest] + shift) % values.shape[longest]
        spots.append(tuple(where))
    return values.at[spots[0]].set(least).at[spots[1]].set(top_value)


def shard_levels(rng, dims, split, smallest, high):
    def one(axis_at, shards_of):
        heights = jax.random.uniform(jax.random.fold_in(jax.random.fold_in(rng, 6), axis_at), (shards_of,), jnp.float32, smallest / len(split), high / len(split))
        return jnp.repeat(jnp.exp(heights), dims[axis_at] // shards_of).reshape((-1,) + (1,) * (len(dims) - axis_at - 1))

    factor_of = one(*split[0])
    for cut in split[1:]:
        factor_of = factor_of * one(*cut)
    return factor_of


def normal_values(stream_key, dims, width, most, shards=(), dtype=jnp.bfloat16):
    loudness = shard_levels(stream_key, dims, shards, -0.22, 0.18) if shards else 1.0
    values = jax.random.normal(stream_key, dims, jnp.float32) * width * loudness
    return jnp.minimum(jnp.maximum(values, -most), most).astype(dtype)


def setup_inputs(seed: int = 0) -> dict:
    splits = jax.random.split(jax.random.key(seed), 10)
    increment = normal_values(splits[0], (WINDOW_PIECES, 3, LEVELS, GX, GY), 1.0, 6.0, ((0, 8), (2, 4)), jnp.float32)
    multiplier = normal_values(splits[1], (WINDOW_PIECES, 3, LEVELS, GX, GY), 1.0, 6.0, ((0, 8), (2, 4)), jnp.float32)
    error_var = jnp.clip(jnp.exp(math.log(1.0) - 2.3025851 * jax.random.uniform(splits[2], (WINDOW_PIECES, 3, LEVELS, GX, GY), jnp.float32) ** shard_levels(splits[2], (WINDOW_PIECES, 3, LEVELS, GX, GY), ((0, 8), (2, 4)), -0.2, 0.2)), 0.1, 1.0)
    obs_cell = set_ends(jax.random.randint(splits[3], (WINDOW_PIECES, LEVELS, NOBS), 0, GX * GY), jax.random.fold_in(splits[3], 1), 0, (GX * GY) - 1).astype(jnp.int32)
    obs_dual = normal_values(splits[4], (WINDOW_PIECES, LEVELS, NOBS), 1.0, 6.0, ((0, 8), (1, 4)), jnp.float32)
    obs_var = jnp.clip(jnp.exp(math.log(2.0) - 1.3862944 * jax.random.uniform(splits[5], (WINDOW_PIECES, LEVELS, NOBS), jnp.float32) ** shard_levels(splits[5], (WINDOW_PIECES, LEVELS, NOBS), ((0, 8), (1, 4)), -0.2, 0.2)), 0.5, 2.0)
    level_gain = jnp.clip(0.5 + 1.0 * jax.random.uniform(splits[6], (LEVELS,), jnp.float32) ** shard_levels(splits[6], (LEVELS,), ((0, 4),), -0.2, 0.2), 0.5, 1.5)
    mean_depth = jnp.clip(jnp.exp(math.log(2.0) - 1.3862944 * jax.random.uniform(splits[7], (LEVELS,), jnp.float32) ** shard_levels(splits[7], (LEVELS,), ((0, 4),), -0.2, 0.2)), 0.5, 2.0)
    chain_decay = draw_chain_decay(jax.random.fold_in(splits[9], 71), 0)
    return dict(increment=increment, multiplier=multiplier, error_var=error_var, obs_cell=obs_cell, obs_dual=obs_dual, obs_var=obs_var, level_gain=level_gain, mean_depth=mean_depth, chain_decay=chain_decay)


TIME_STEP = 0.25
ROTATION_PARAM = 0.5
COUPLING = 0.25

def dynamics_advance(state, column, level_gain, mean_depth):
    h, u, v = (state[0], state[1], state[2])
    p = level_gain[:, None, None] * h + COUPLING * column[None]
    gradient_eastward = jnp.concatenate([p[:, 1:, :], jnp.zeros_like(p[:, :1, :])], axis=1) - p
    grad_y = jnp.concatenate([p[:, :, 1:], jnp.zeros_like(p[:, :, :1])], axis=2) - p
    u_new = u + TIME_STEP * (ROTATION_PARAM * v - gradient_eastward)
    v_new = v - TIME_STEP * (ROTATION_PARAM * u + grad_y)
    back_x = u_new - jnp.concatenate([jnp.zeros_like(u_new[:, :1, :]), u_new[:, :-1, :]], axis=1)
    back_y = v_new - jnp.concatenate([jnp.zeros_like(v_new[:, :, :1]), v_new[:, :, :-1]], axis=2)
    h_new = h - TIME_STEP * mean_depth[:, None, None] * (back_x + back_y)
    return jnp.stack([h_new, u_new, v_new])

def reference(increment, multiplier, error_var, obs_cell, obs_dual, obs_var, level_gain, mean_depth, chain_decay):

    def advance(state):
        for step in range(STEPS):
            state = dynamics_advance(state, lax.optimization_barrier(jnp.sum(state[0], axis=0)), level_gain, mean_depth)
        return state

    def flip_matrix(state):
        return jax.vjp(advance, state)[1](state)[0]
    advanced = lax.map(advance, increment)
    returned = lax.map(flip_matrix, multiplier)
    forward_term = jnp.concatenate([jnp.zeros_like(advanced[:1]), advanced[:-1]], axis=0)
    backward_term = jnp.concatenate([returned[1:], jnp.zeros_like(returned[:1])], axis=0)
    dual_product = error_var * multiplier + increment - forward_term
    flat_h = increment[:, 0].reshape(WINDOW_PIECES, LEVELS, GX * GY)
    picked = jnp.take_along_axis(flat_h, obs_cell, axis=2)
    obs_product = obs_var * obs_dual + picked

    def spread(cells, values):
        return jnp.zeros((GX * GY,), jnp.float32).at[cells].add(values)
    added = jax.vmap(jax.vmap(spread))(obs_cell, obs_dual).reshape(WINDOW_PIECES, LEVELS, GX, GY)
    state_block_product = multiplier - backward_term
    state_block_product = state_block_product.at[:, 0].add(added)

    def recur(carry, inputs):
        scale_multiplier, value = inputs
        result = scale_multiplier[:, :, None, None] * carry + value
        return (result, result)
    first = jnp.zeros_like(dual_product[0])
    unused, chain_solution = lax.scan(recur, first, (chain_decay, dual_product))
    return (dual_product, obs_product, state_block_product, chain_solution)
```

```python
import functools

import jax
import jax.numpy as jnp
from jax import lax
from jax.experimental import pallas as pl
from jax.experimental.pallas import tpu as pltpu
from jax.sharding import PartitionSpec as P

TIME_STEP = 0.25
ROTATION_PARAM = 0.5
COUPLING = 0.25
SPLIT = 2
MESH_ID = pl.DeviceIdType.MESH


def up(a, axis):
    n = a.shape[axis]
    tail = lax.slice_in_dim(a, 1, n, axis=axis)
    return jnp.concatenate([tail, jnp.zeros_like(lax.slice_in_dim(a, 0, 1, axis=axis))], axis=axis)


def down(a, axis):
    n = a.shape[axis]
    head = lax.slice_in_dim(a, 0, n - 1, axis=axis)
    return jnp.concatenate([jnp.zeros_like(lax.slice_in_dim(a, 0, 1, axis=axis)), head], axis=axis)


def diff_x(a):
    return up(a, a.ndim - 2) - a


def diff_y(a):
    return up(a, a.ndim - 1) - a


def back_x(a):
    return a - down(a, a.ndim - 2)


def back_y(a):
    return a - down(a, a.ndim - 1)


def step_forward(h, u, v, column, gain, depth):
    p = gain * h
    if column is not None:
        p = p + COUPLING * column[None]
    u_new = u + TIME_STEP * (ROTATION_PARAM * v - diff_x(p))
    v_new = v - TIME_STEP * (ROTATION_PARAM * u + diff_y(p))
    h_new = h - TIME_STEP * depth * (back_x(u_new) + back_y(v_new))
    return h_new, u_new, v_new


def step_back(h, u, v, gain, depth):
    w = depth * h
    u2 = u + TIME_STEP * diff_x(w)
    v2 = v + TIME_STEP * diff_y(w)
    p = TIME_STEP * (back_x(u2) + back_y(v2))
    half = TIME_STEP * ROTATION_PARAM
    return h + gain * p, u2 - half * v2, v2 + half * u2, COUPLING * jnp.sum(p, axis=0)


def second_column(pair, total_depth):
    c = pair[0]
    lap = back_x(diff_x(c)) + back_y(diff_y(c))
    return jnp.stack([c, pair[1] + (TIME_STEP * TIME_STEP * COUPLING) * total_depth * lap])


def sum_fields(fields_a, fields_b, depth_sum):
    size = lax.axis_size("lev")
    if size < 2 or size & (size - 1):
        total_depth = lax.psum(depth_sum, "lev")
        a, b = lax.psum((fields_a, fields_b), "lev")
        return second_column(a, total_depth), second_column(b, total_depth)

    def swap(x, bit):
        return lax.ppermute(x, "lev", [(i, i ^ bit) for i in range(size)])

    total_depth = depth_sum
    bit = 1
    while bit < size:
        total_depth = total_depth + swap(total_depth, bit)
        bit *= 2
    first = lax.axis_index("lev") % 2 == 0
    kept = jnp.where(first, fields_a, fields_b)
    given = jnp.where(first, fields_b, fields_a)
    kept = kept + swap(given, 1)
    bit = 2
    while bit < size:
        kept = kept + swap(kept, bit)
        bit *= 2
    kept = second_column(kept, total_depth[0])
    other = swap(kept, 1)
    return jnp.where(first, kept, other), jnp.where(first, other, kept)


def chain_kernel(
    n, chunks, per, scale, tangent, own, partner, adjoint,
    dual, chain, adjoint_in, tangent_in, carried, sent,
    t_send, t_recv, m_send, m_recv, c_send, c_recv,
):
    s = lax.axis_index("tm")
    odd = (s % 2).astype(jnp.float32)

    def remote(src, dst, send, recv, to):
        return pltpu.make_async_remote_copy(
            src_ref=src, dst_ref=dst, send_sem=send, recv_sem=recv,
            device_id={"tm": to}, device_id_type=MESH_ID,
        )

    def tangent_copy(c):
        return remote(tangent.at[c], tangent_in.at[c], t_send.at[c], t_recv.at[c], s + 1)

    def adjoint_copy(c):
        return remote(adjoint.at[c], adjoint_in.at[c], m_send.at[c], m_recv.at[c], s - 1)

    def chain_copy(c):
        return remote(sent.at[c], carried.at[c], c_send.at[c], c_recv.at[c], s + 2)

    def every(fn):
        lax.fori_loop(0, chunks, lambda c, z: (fn(c), z)[1], 0)

    barrier = pltpu.get_barrier_semaphore()
    near = ((s >= 1, s - 1), (s >= 2, s - 2), (s < n - 1, s + 1), (s < n - 2, s + 2))
    for there, who in near:
        @pl.when(there)
        def _():
            pl.semaphore_signal(barrier, inc=1, device_id={"tm": who}, device_id_type=MESH_ID)
    pl.semaphore_wait(barrier, sum(there.astype(jnp.int32) for there, _ in near))

    @pl.when(s < n - 1)
    def _():
        every(lambda c: tangent_copy(c).start())

    @pl.when(s >= 1)
    def _():
        every(lambda c: adjoint_copy(c).start())

    def one(c):
        d = scale[0, c // per]
        d_next = scale[1, c // per]

        @pl.when(s >= 1)
        def _():
            tangent_copy(c).wait_recv()

        @pl.when(s == 0)
        def _():
            tangent_in[c] = jnp.zeros(tangent_in.shape[1:], jnp.float32)

        @pl.when(s >= 2)
        def _():
            chain_copy(c).wait_recv()

        @pl.when(s < 2)
        def _():
            carried[c] = jnp.zeros(carried.shape[1:], jnp.float32)

        swap = partner[c]
        dual_here = own[c] - tangent_in[c]
        here = d * (carried[c] + odd * swap) + dual_here
        sent[c] = d_next * here + ((1.0 - odd) * swap - tangent[c])

        @pl.when(s < n - 2)
        def _():
            chain_copy(c).start()

        dual[c] = dual_here
        chain[c] = here

    every(one)

    @pl.when(s < n - 1)
    def _():
        every(lambda c: tangent_copy(c).wait_send())
        every(lambda c: adjoint_copy(c).wait_recv())

    @pl.when(s == n - 1)
    def _():
        adjoint_in[...] = jnp.zeros_like(adjoint_in)

    @pl.when(s >= 1)
    def _():
        every(lambda c: adjoint_copy(c).wait_send())

    @pl.when(s < n - 2)
    def _():
        every(lambda c: chain_copy(c).wait_send())


def run_chain(scale, tangent, own, partner, adjoint):
    n = lax.axis_size("tm")
    planes, rows, cols = tangent.shape
    per = SPLIT if rows % (8 * SPLIT) == 0 else 1
    chunks = planes * per
    shape = (chunks, rows // per, cols)
    arrays = [a.reshape(shape) for a in (tangent, own, partner, adjoint)]
    vmem = pl.BlockSpec(memory_space=pltpu.VMEM)
    out = jax.ShapeDtypeStruct(shape, jnp.float32)
    results = pl.pallas_call(
        functools.partial(chain_kernel, n, chunks, per),
        out_shape=[out] * 3,
        in_specs=[pl.BlockSpec(memory_space=pltpu.SMEM)] + [vmem] * 4,
        out_specs=[vmem] * 3,
        scratch_shapes=[pltpu.VMEM(shape, jnp.float32)] * 3
        + [pltpu.SemaphoreType.DMA((chunks,))] * 6,
        compiler_params=pltpu.CompilerParams(
            collective_id=0, has_side_effects=True, vmem_limit_bytes=56 * 1024 * 1024
        ),
        cost_estimate=pl.CostEstimate(
            flops=20 * tangent.size, bytes_accessed=40 * tangent.size, transcendentals=0
        ),
    )(scale, *arrays)
    return [r.reshape(tangent.shape) for r in results]


def shards(
    increment, multiplier, error_var, obs_cell, obs_dual, obs_var,
    level_gain, mean_depth, chain_decay,
):
    n = lax.axis_size("tm")
    state = increment[0]
    dual = multiplier[0]
    fields, levels, rows, cols = state.shape
    gain = level_gain[:, None, None]
    depth = mean_depth[:, None, None]

    own = error_var[0] * dual + state
    own, state, dual = lax.optimization_barrier((own, state, dual))
    pairs = [(i, i ^ 1) for i in range(n) if i ^ 1 < n]
    partner = lax.ppermute(own, "tm", pairs)
    decay = chain_decay[0].reshape(-1)
    decay_next = lax.ppermute(decay, "tm", [(i, i - 1) for i in range(1, n)])

    first = step_forward(state[0], state[1], state[2], None, gain, depth)
    ahead = jnp.stack([jnp.sum(state[0], axis=0), jnp.sum(first[0], axis=0)])
    b1 = step_back(dual[0], dual[1], dual[2], gain, depth)
    b2 = step_back(b1[0], b1[1], b1[2], gain, depth)
    behind = jnp.stack([b1[3], b2[3]])
    columns, bars = sum_fields(ahead, behind, jnp.sum(mean_depth, keepdims=True))

    t = step_forward(state[0], state[1], state[2], columns[0], gain, depth)
    t = step_forward(t[0], t[1], t[2], columns[1], gain, depth)
    r = step_back(b1[0] + bars[0][None], b1[1], b1[2], gain, depth)
    r = (r[0] + bars[1][None], r[1], r[2])

    flat = (fields * levels, rows, cols)
    dual_product, chain_solution, returned = run_chain(
        jnp.stack([decay, decay_next]),
        jnp.stack(t).reshape(flat), own.reshape(flat), partner.reshape(flat),
        jnp.stack(r).reshape(flat),
    )

    flat_h = state[0].reshape(levels, -1)
    picked = jnp.take_along_axis(flat_h, obs_cell[0], axis=1)
    obs_product = obs_var[0] * obs_dual[0] + picked

    def spread(cells, values):
        return jnp.zeros((flat_h.shape[1],), jnp.float32).at[cells].add(values)

    added = jax.vmap(spread)(obs_cell[0], obs_dual[0]).reshape(state[0].shape)
    state_block = (dual - returned.reshape(state.shape)).at[0].add(added)
    return (
        dual_product.reshape(increment.shape), obs_product[None],
        state_block[None], chain_solution.reshape(increment.shape),
    )


def solution(mesh):
    state = P("tm", None, "lev", None, None)
    obs = P("tm", "lev", None)
    return jax.shard_map(
        shards,
        mesh=mesh,
        in_specs=(state, state, state, obs, obs, obs, P("lev"), P("lev"), P("tm", None, "lev")),
        out_specs=(state, obs, state, state),
        check_vma=False,
    )
```

```python
import functools

import jax
import jax.numpy as jnp
from jax import lax
from jax.experimental import pallas as pl
from jax.experimental.pallas import tpu as pltpu
from jax.sharding import PartitionSpec as P


TIME_STEP = 0.25
ROTATION_PARAM = 0.5
COUPLING = 0.25
SPLIT = 2
MESH_ID = pl.DeviceIdType.MESH


def up(a, axis):
    n = a.shape[axis]
    tail = lax.slice_in_dim(a, 1, n, axis=axis)
    return jnp.concatenate([tail, jnp.zeros_like(lax.slice_in_dim(a, 0, 1, axis=axis))], axis=axis)


def down(a, axis):
    n = a.shape[axis]
    head = lax.slice_in_dim(a, 0, n - 1, axis=axis)
    return jnp.concatenate([jnp.zeros_like(lax.slice_in_dim(a, 0, 1, axis=axis)), head], axis=axis)


def diff_x(a):
    return up(a, a.ndim - 2) - a


def diff_y(a):
    return up(a, a.ndim - 1) - a


def back_x(a):
    return a - down(a, a.ndim - 2)


def back_y(a):
    return a - down(a, a.ndim - 1)


def step_forward(h, u, v, column, gain, depth):
    p = gain * h
    if column is not None:
        p = p + COUPLING * column[None]
    u_new = u + TIME_STEP * (ROTATION_PARAM * v - diff_x(p))
    v_new = v - TIME_STEP * (ROTATION_PARAM * u + diff_y(p))
    h_new = h - TIME_STEP * depth * (back_x(u_new) + back_y(v_new))
    return h_new, u_new, v_new


def step_back(h, u, v, gain, depth):
    w = depth * h
    u2 = u + TIME_STEP * diff_x(w)
    v2 = v + TIME_STEP * diff_y(w)
    p = TIME_STEP * (back_x(u2) + back_y(v2))
    half = TIME_STEP * ROTATION_PARAM
    return h + gain * p, u2 - half * v2, v2 + half * u2, COUPLING * jnp.sum(p, axis=0)


def second_column(pair, total_depth):
    c = pair[0]
    lap = back_x(diff_x(c)) + back_y(diff_y(c))
    return jnp.stack([c, pair[1] + (TIME_STEP * TIME_STEP * COUPLING) * total_depth * lap])


def sum_fields(fields_a, fields_b, depth_sum):
    size = lax.axis_size("lev")
    if size < 2 or size & (size - 1):
        total_depth = lax.psum(depth_sum, "lev")
        a, b = lax.psum((fields_a, fields_b), "lev")
        return second_column(a, total_depth), second_column(b, total_depth)

    def swap(x, bit):
        return lax.ppermute(x, "lev", [(i, i ^ bit) for i in range(size)])

    shape = fields_a.shape
    cols = shape[-1]
    depths = jnp.zeros((8, cols), jnp.float32) + depth_sum

    def packed(fields):
        return jnp.concatenate([fields.reshape(-1, cols), depths], axis=0)

    first = lax.axis_index("lev") % 2 == 0
    kept = packed(jnp.where(first, fields_a, fields_b))
    given = packed(jnp.where(first, fields_b, fields_a))
    met = swap(given, 1)
    kept = kept + met
    bit = 2
    while bit < size:
        met = swap(kept, bit)
        kept = kept + met
        bit *= 2
    done = second_column(kept[:-8].reshape(shape), kept[-1:, :1])
    other = swap(done, 1)
    return jnp.where(first, done, other), jnp.where(first, other, done)


def chain_kernel(
    n, chunks, per, scale, tangent, own, partner, adjoint,
    dual, chain, adjoint_in,
    tangent_here, own_here, partner_here, tangent_in, carried, sent, dual_here, chain_here,
    t_send, t_recv, m_send, m_recv, c_send, c_recv, d_out, s_out, loads,
):
    s = lax.axis_index("tm")
    odd = (s % 2).astype(jnp.float32)

    def remote(src, dst, send, recv, to):
        return pltpu.make_async_remote_copy(
            src_ref=src, dst_ref=dst, send_sem=send, recv_sem=recv,
            device_id={"tm": to}, device_id_type=MESH_ID,
        )

    def tangent_copy(c):
        return remote(tangent.at[c], tangent_in.at[c], t_send.at[c], t_recv.at[c], s + 1)

    def adjoint_copy(c):
        return remote(adjoint.at[c], adjoint_in.at[c], m_send.at[c], m_recv.at[c], s - 1)

    def chain_copy(c):
        return remote(sent.at[c], carried.at[c], c_send.at[c], c_recv.at[c], s + 2)

    def every(fn):
        lax.fori_loop(0, chunks, lambda c, z: (fn(c), z)[1], 0)

    def dual_copy(c):
        return pltpu.make_async_copy(dual_here.at[c], dual.at[c], d_out.at[c])

    def solution_copy(c):
        return pltpu.make_async_copy(chain_here.at[c], chain.at[c], s_out.at[c])

    fetched = [
        pltpu.make_async_copy(tangent, tangent_here, loads.at[0]),
        pltpu.make_async_copy(own, own_here, loads.at[1]),
        pltpu.make_async_copy(partner, partner_here, loads.at[2]),
    ]
    barrier = pltpu.get_barrier_semaphore()
    near = ((s >= 1, s - 1), (s >= 2, s - 2), (s < n - 1, s + 1), (s < n - 2, s + 2))
    for there, who in near:
        @pl.when(there)
        def _():
            pl.semaphore_signal(barrier, inc=1, device_id={"tm": who}, device_id_type=MESH_ID)
    pl.semaphore_wait(barrier, sum(there.astype(jnp.int32) for there, _ in near))

    @pl.when(s < n - 1)
    def _():
        every(lambda c: tangent_copy(c).start())

    @pl.when(s >= 1)
    def _():
        every(lambda c: adjoint_copy(c).start())

    for copy in fetched:
        copy.start()
    for copy in fetched:
        copy.wait()

    def one(c):
        d = scale[0, c // per]
        d_next = scale[1, c // per]

        @pl.when(s >= 1)
        def _():
            tangent_copy(c).wait_recv()

        @pl.when(s == 0)
        def _():
            tangent_in[c] = jnp.zeros(tangent_in.shape[1:], jnp.float32)

        @pl.when(s >= 2)
        def _():
            chain_copy(c).wait_recv()

        @pl.when(s < 2)
        def _():
            carried[c] = jnp.zeros(carried.shape[1:], jnp.float32)

        swap = partner_here[c]
        product_here = own_here[c] - tangent_in[c]
        here = d * (carried[c] + odd * swap) + product_here
        sent[c] = d_next * here + ((1.0 - odd) * swap - tangent_here[c])

        @pl.when(s < n - 2)
        def _():
            chain_copy(c).start()

        dual_here[c] = product_here
        chain_here[c] = here
        dual_copy(c).start()
        solution_copy(c).start()

    every(one)

    @pl.when(s < n - 1)
    def _():
        every(lambda c: tangent_copy(c).wait_send())
        every(lambda c: adjoint_copy(c).wait_recv())

    every(lambda c: dual_copy(c).wait())
    every(lambda c: solution_copy(c).wait())

    @pl.when(s >= 1)
    def _():
        every(lambda c: adjoint_copy(c).wait_send())

    @pl.when(s < n - 2)
    def _():
        every(lambda c: chain_copy(c).wait_send())


def run_chain(scale, tangent, own, partner, adjoint):
    n = lax.axis_size("tm")
    planes, rows, cols = tangent.shape
    per = SPLIT if rows % (8 * SPLIT) == 0 else 1
    chunks = planes * per
    shape = (chunks, rows // per, cols)
    arrays = [a.reshape(shape) for a in (tangent, own, partner, adjoint)]
    place = pl.BlockSpec(memory_space=pl.ANY)
    out = jax.ShapeDtypeStruct(shape, jnp.float32)
    results = pl.pallas_call(
        functools.partial(chain_kernel, n, chunks, per),
        out_shape=[out] * 3,
        in_specs=[pl.BlockSpec(memory_space=pltpu.SMEM)] + [place] * 4,
        out_specs=[place] * 3,
        scratch_shapes=[pltpu.VMEM(shape, jnp.float32)] * 8
        + [pltpu.SemaphoreType.DMA((chunks,))] * 8
        + [pltpu.SemaphoreType.DMA((3,))],
        compiler_params=pltpu.CompilerParams(
            collective_id=0, has_side_effects=True, vmem_limit_bytes=56 * 1024 * 1024
        ),
        cost_estimate=pl.CostEstimate(
            flops=20 * tangent.size, bytes_accessed=40 * tangent.size, transcendentals=0
        ),
    )(scale, *arrays)
    return [r.reshape(tangent.shape) for r in results]


def product(
    increment, multiplier, error_var, obs_cell, obs_dual, obs_var,
    level_gain, mean_depth, chain_decay,
):
    n = lax.axis_size("tm")
    state = increment[0]
    dual = multiplier[0]
    fields, levels, rows, cols = state.shape
    gain = level_gain[:, None, None]
    depth = mean_depth[:, None, None]

    own = error_var[0] * dual + state
    own, state, dual = lax.optimization_barrier((own, state, dual))
    pairs = [(i, i ^ 1) for i in range(n) if i ^ 1 < n]
    partner = lax.ppermute(own, "tm", pairs)
    decay = chain_decay[0].reshape(-1)
    decay_next = lax.ppermute(decay, "tm", [(i, i - 1) for i in range(1, n)])

    first = step_forward(state[0], state[1], state[2], None, gain, depth)
    ahead = jnp.stack([jnp.sum(state[0], axis=0), jnp.sum(first[0], axis=0)])
    b1 = step_back(dual[0], dual[1], dual[2], gain, depth)
    b2 = step_back(b1[0], b1[1], b1[2], gain, depth)
    behind = jnp.stack([b1[3], b2[3]])
    columns, bars = sum_fields(ahead, behind, jnp.sum(mean_depth, keepdims=True))

    t = step_forward(state[0], state[1], state[2], columns[0], gain, depth)
    t = step_forward(t[0], t[1], t[2], columns[1], gain, depth)
    r = step_back(b1[0] + bars[0][None], b1[1], b1[2], gain, depth)
    r = (r[0] + bars[1][None], r[1], r[2])

    flat = (fields * levels, rows, cols)
    dual_product, chain_solution, returned = run_chain(
        jnp.stack([decay, decay_next]),
        jnp.stack(t).reshape(flat), own.reshape(flat), partner.reshape(flat),
        jnp.stack(r).reshape(flat),
    )

    flat_h = increment[0, 0].reshape(levels, -1)
    picked = jnp.take_along_axis(flat_h, obs_cell[0], axis=1)
    obs_product = obs_var[0] * obs_dual[0] + picked

    def spread(cells, values):
        return jnp.zeros((flat_h.shape[1],), jnp.float32).at[cells].add(values)

    added = jax.vmap(spread)(obs_cell[0], obs_dual[0]).reshape(state[0].shape)
    returned = jnp.where(lax.axis_index("tm") < n - 1, returned.reshape(state.shape), 0.0)
    state_block = (dual - returned).at[0].add(added)
    return (
        dual_product.reshape(increment.shape), obs_product[None],
        state_block[None], chain_solution.reshape(increment.shape),
    )


def solution(mesh):
    state = P("tm", None, "lev", None, None)
    obs = P("tm", "lev", None)
    return jax.shard_map(
        product,
        mesh=mesh,
        in_specs=(state, state, state, obs, obs, obs, P("lev"), P("lev"), P("tm", None, "lev")),
        out_specs=(state, obs, state, state),
        check_vma=False,
    )
```

```python
import functools

import jax
import jax.numpy as jnp
from jax import lax
from jax.experimental import pallas as pl
from jax.experimental.pallas import tpu as pltpu
from jax.sharding import PartitionSpec as P


TIME_STEP = 0.25
ROTATION_PARAM = 0.5
COUPLING = 0.25
SPLIT = 2
MESH_ID = pl.DeviceIdType.MESH


def up(a, axis):
    n = a.shape[axis]
    tail = lax.slice_in_dim(a, 1, n, axis=axis)
    return jnp.concatenate([tail, jnp.zeros_like(lax.slice_in_dim(a, 0, 1, axis=axis))], axis=axis)


def down(a, axis):
    n = a.shape[axis]
    head = lax.slice_in_dim(a, 0, n - 1, axis=axis)
    return jnp.concatenate([jnp.zeros_like(lax.slice_in_dim(a, 0, 1, axis=axis)), head], axis=axis)


def diff_x(a):
    return up(a, a.ndim - 2) - a


def diff_y(a):
    return up(a, a.ndim - 1) - a


def back_x(a):
    return a - down(a, a.ndim - 2)


def back_y(a):
    return a - down(a, a.ndim - 1)


def step_forward(h, u, v, column, gain, depth):
    p = gain * h
    if column is not None:
        p = p + COUPLING * column[None]
    u_new = u + TIME_STEP * (ROTATION_PARAM * v - diff_x(p))
    v_new = v - TIME_STEP * (ROTATION_PARAM * u + diff_y(p))
    h_new = h - TIME_STEP * depth * (back_x(u_new) + back_y(v_new))
    return h_new, u_new, v_new


def step_back(h, u, v, gain, depth):
    w = depth * h
    u2 = u + TIME_STEP * diff_x(w)
    v2 = v + TIME_STEP * diff_y(w)
    p = TIME_STEP * (back_x(u2) + back_y(v2))
    half = TIME_STEP * ROTATION_PARAM
    return h + gain * p, u2 - half * v2, v2 + half * u2, COUPLING * jnp.sum(p, axis=0)


def second_column(pair, total_depth):
    c = pair[0]
    lap = back_x(diff_x(c)) + back_y(diff_y(c))
    return jnp.stack([c, pair[1] + (TIME_STEP * TIME_STEP * COUPLING) * total_depth * lap])


def sum_fields(fields_a, fields_b, depth_sum, beside):
    size = lax.axis_size("lev")
    if size < 2 or size & (size - 1):
        total_depth = lax.psum(depth_sum, "lev")
        a, b = lax.psum((fields_a, fields_b), "lev")
        return second_column(a, total_depth), second_column(b, total_depth), beside

    def swap(x, bit):
        return lax.ppermute(x, "lev", [(i, i ^ bit) for i in range(size)])

    shape = fields_a.shape
    cols = shape[-1]
    depths = jnp.zeros((8, cols), jnp.float32) + depth_sum

    def packed(fields):
        return jnp.concatenate([fields.reshape(-1, cols), depths], axis=0)

    first = lax.axis_index("lev") % 2 == 0
    kept = packed(jnp.where(first, fields_a, fields_b))
    given = packed(jnp.where(first, fields_b, fields_a))
    met = swap(given, 1)
    kept = kept + met
    bit = 2
    while bit < size:
        met = swap(kept, bit)
        met, beside = lax.optimization_barrier((met, beside))
        kept = kept + met
        bit *= 2
    done = second_column(kept[:-8].reshape(shape), kept[-1:, :1])
    other = swap(done, 1)
    return jnp.where(first, done, other), jnp.where(first, other, done), beside


def chain_kernel(
    n, chunks, per, scale, tangent, own, partner, adjoint,
    dual, chain, adjoint_in,
    tangent_here, own_here, partner_here, tangent_in, carried, sent, dual_here, chain_here,
    t_send, t_recv, m_send, m_recv, c_send, c_recv, d_out, s_out, loads,
):
    s = lax.axis_index("tm")
    odd = (s % 2).astype(jnp.float32)

    def remote(src, dst, send, recv, to):
        return pltpu.make_async_remote_copy(
            src_ref=src, dst_ref=dst, send_sem=send, recv_sem=recv,
            device_id={"tm": to}, device_id_type=MESH_ID,
        )

    def tangent_copy(c):
        return remote(tangent.at[c], tangent_in.at[c], t_send.at[c], t_recv.at[c], s + 1)

    def adjoint_copy(c):
        return remote(adjoint.at[c], adjoint_in.at[c], m_send.at[c], m_recv.at[c], s - 1)

    def chain_copy(c):
        return remote(sent.at[c], carried.at[c], c_send.at[c], c_recv.at[c], s + 2)

    def every(fn):
        lax.fori_loop(0, chunks, lambda c, z: (fn(c), z)[1], 0)

    def dual_copy(c):
        return pltpu.make_async_copy(dual_here.at[c], dual.at[c], d_out.at[c])

    def solution_copy(c):
        return pltpu.make_async_copy(chain_here.at[c], chain.at[c], s_out.at[c])

    fetched = [
        pltpu.make_async_copy(tangent, tangent_here, loads.at[0]),
        pltpu.make_async_copy(own, own_here, loads.at[1]),
        pltpu.make_async_copy(partner, partner_here, loads.at[2]),
    ]
    barrier = pltpu.get_barrier_semaphore()
    near = ((s >= 1, s - 1), (s >= 2, s - 2), (s < n - 1, s + 1), (s < n - 2, s + 2))
    for there, who in near:
        @pl.when(there)
        def _():
            pl.semaphore_signal(barrier, inc=1, device_id={"tm": who}, device_id_type=MESH_ID)
    pl.semaphore_wait(barrier, sum(there.astype(jnp.int32) for there, _ in near))

    @pl.when(s < n - 1)
    def _():
        every(lambda c: tangent_copy(c).start())

    @pl.when(s >= 1)
    def _():
        every(lambda c: adjoint_copy(c).start())

    for copy in fetched:
        copy.start()
    for copy in fetched:
        copy.wait()

    def one(c):
        d = scale[0, c // per]
        d_next = scale[1, c // per]

        @pl.when(s >= 1)
        def _():
            tangent_copy(c).wait_recv()

        @pl.when(s == 0)
        def _():
            tangent_in[c] = jnp.zeros(tangent_in.shape[1:], jnp.float32)

        @pl.when(s >= 2)
        def _():
            chain_copy(c).wait_recv()

        @pl.when(s < 2)
        def _():
            carried[c] = jnp.zeros(carried.shape[1:], jnp.float32)

        swap = partner_here[c]
        product_here = own_here[c] - tangent_in[c]
        here = d * (carried[c] + odd * swap) + product_here
        sent[c] = d_next * here + ((1.0 - odd) * swap - tangent_here[c])

        @pl.when(s < n - 2)
        def _():
            chain_copy(c).start()

        dual_here[c] = product_here
        chain_here[c] = here
        dual_copy(c).start()
        solution_copy(c).start()

    every(one)

    @pl.when(s < n - 1)
    def _():
        every(lambda c: tangent_copy(c).wait_send())
        every(lambda c: adjoint_copy(c).wait_recv())

    every(lambda c: dual_copy(c).wait())
    every(lambda c: solution_copy(c).wait())

    @pl.when(s >= 1)
    def _():
        every(lambda c: adjoint_copy(c).wait_send())

    @pl.when(s < n - 2)
    def _():
        every(lambda c: chain_copy(c).wait_send())


def run_chain(scale, tangent, own, partner, adjoint):
    n = lax.axis_size("tm")
    planes, rows, cols = tangent.shape
    per = SPLIT if rows % (8 * SPLIT) == 0 else 1
    chunks = planes * per
    shape = (chunks, rows // per, cols)
    arrays = [a.reshape(shape) for a in (tangent, own, partner, adjoint)]
    place = pl.BlockSpec(memory_space=pl.ANY)
    out = jax.ShapeDtypeStruct(shape, jnp.float32)
    results = pl.pallas_call(
        functools.partial(chain_kernel, n, chunks, per),
        out_shape=[out] * 3,
        in_specs=[pl.BlockSpec(memory_space=pltpu.SMEM)] + [place] * 4,
        out_specs=[place] * 3,
        scratch_shapes=[pltpu.VMEM(shape, jnp.float32)] * 8
        + [pltpu.SemaphoreType.DMA((chunks,))] * 8
        + [pltpu.SemaphoreType.DMA((3,))],
        compiler_params=pltpu.CompilerParams(
            collective_id=0, has_side_effects=True, vmem_limit_bytes=56 * 1024 * 1024
        ),
        cost_estimate=pl.CostEstimate(
            flops=20 * tangent.size, bytes_accessed=40 * tangent.size, transcendentals=0
        ),
    )(scale, *arrays)
    return [r.reshape(tangent.shape) for r in results]


def product(
    increment, multiplier, error_var, obs_cell, obs_dual, obs_var,
    level_gain, mean_depth, chain_decay,
):
    n = lax.axis_size("tm")
    state = increment[0]
    dual = multiplier[0]
    fields, levels, rows, cols = state.shape
    gain = level_gain[:, None, None]
    depth = mean_depth[:, None, None]

    own = error_var[0] * dual + state
    own, state, dual = lax.optimization_barrier((own, state, dual))
    pairs = [(i, i ^ 1) for i in range(n) if i ^ 1 < n]
    partner = lax.ppermute(own, "tm", pairs)
    decay = chain_decay[0].reshape(-1)
    decay_next = lax.ppermute(decay, "tm", [(i, i - 1) for i in range(1, n)])

    flat_h = increment[0, 0].reshape(levels, -1)
    picked = jnp.take_along_axis(flat_h, obs_cell[0], axis=1)
    obs_product = obs_var[0] * obs_dual[0] + picked

    def spread(cells, values):
        return jnp.zeros((flat_h.shape[1],), jnp.float32).at[cells].add(values)

    added = jax.vmap(spread)(obs_cell[0], obs_dual[0]).reshape(state[0].shape)
    first = step_forward(state[0], state[1], state[2], None, gain, depth)
    ahead = jnp.stack([jnp.sum(state[0], axis=0), jnp.sum(first[0], axis=0)])
    b1 = step_back(dual[0], dual[1], dual[2], gain, depth)
    b2 = step_back(b1[0], b1[1], b1[2], gain, depth)
    behind = jnp.stack([b1[3], b2[3]])
    columns, bars, added = sum_fields(
        ahead, behind, jnp.sum(mean_depth, keepdims=True), added
    )

    t = step_forward(state[0], state[1], state[2], columns[0], gain, depth)
    t = step_forward(t[0], t[1], t[2], columns[1], gain, depth)
    r = step_back(b1[0] + bars[0][None], b1[1], b1[2], gain, depth)
    r = (r[0] + bars[1][None], r[1], r[2])

    flat = (fields * levels, rows, cols)
    dual_product, chain_solution, returned = run_chain(
        jnp.stack([decay, decay_next]),
        jnp.stack(t).reshape(flat), own.reshape(flat), partner.reshape(flat),
        jnp.stack(r).reshape(flat),
    )

    returned = jnp.where(lax.axis_index("tm") < n - 1, returned.reshape(state.shape), 0.0)
    state_block = (dual - returned).at[0].add(added)
    return (
        dual_product.reshape(increment.shape), obs_product[None],
        state_block[None], chain_solution.reshape(increment.shape),
    )


def solution(mesh):
    state = P("tm", None, "lev", None, None)
    obs = P("tm", "lev", None)
    return jax.shard_map(
        product,
        mesh=mesh,
        in_specs=(state, state, state, obs, obs, obs, P("lev"), P("lev"), P("tm", None, "lev")),
        out_specs=(state, obs, state, state),
        check_vma=False,
    )
```
